32 devices in a mesh: row: 4 (over y, core), col: 8 (over z, x).
Axes of the slice: x: 2, y: 2, z: 4, core: 2. Of those that a mesh axis runs over, the one named last changes fastest.
Arguments:
- fluid_data: float32 [51, 8192], P(None, ('row', 'col')), as said below
- center_data: float32 [51, 8192], P(None, ('col', 'row')), as said below
- poly_coef: float32 [48, 4], replicated, may hold values from -3 to 3
Outputs:
- fluid_motion: float32 [48, 8192], P(None, ('row', 'col'))
- center_load: float32 [48, 8192], P(None, ('col', 'row'))
The draws below stay inside these ranges and needn't reach their ends.
Inputs may be any that keep to these rules, and one draw needn't show every extreme that they name: Rows 0 to 2 of fluid_data lie in [0, 1]; rows 3 and on are forces. Rows 0 and 1 of center_data lie in [0, 1] and row 2 lies in [-0.5, -0.02], so every center is at least 0.02 below every vertex; rows 3 and on are coefficients.
All inputs are finite; a program needn't handle non-finite values.
Results may differ from the reference program's by a relative error of at most 0.0003.
Values sent between devices are 32-bit elements; how exact they have to be, the bound alone decides.
A program may use at most 64 MiB of HBM per device.

```python
import math
import jax
import jax.numpy as jnp
from jax import lax

WAVES = 64
COLS = 48
FLUID = 8192
CENTERS = 8192


def draw_fluid_data(key, part):
    first, second = jax.random.split(jax.random.fold_in(key, 11))
    places = jax.random.uniform(first, (3, FLUID), jnp.float32)
    spread = 2.0 * math.pi * WAVES * math.sqrt(0.8 / FLUID)
    values = jax.random.normal(second, (COLS, FLUID), jnp.float32) * spread
    return jnp.concatenate([places, values], axis=0)


def draw_center_data(key, part):
    first, second, third = jax.random.split(jax.random.fold_in(key, 23), 3)
    plane = jax.random.uniform(first, (2, CENTERS), jnp.float32)
    depth = jax.random.uniform(second, (1, CENTERS), jnp.float32)
    spread = 2.0 * math.pi * WAVES * math.sqrt(0.8 / CENTERS)
    height = -0.02 - 0.48 * depth
    values = jax.random.normal(third, (COLS, CENTERS), jnp.float32) * spread
    return jnp.concatenate([plane, height, values], axis=0)


def noise(key, dims, scale, limit, kind=jnp.bfloat16):
    entries = scale * jax.random.normal(key, dims, jnp.float32)
    return jnp.clip(entries, min=-limit, max=limit).astype(kind)


def setup_inputs(seed: int = 0) -> dict:
    streams_of = jax.random.split(jax.random.key(seed), 4)
    fluid_data = draw_fluid_data(jax.random.fold_in(streams_of[3], 71), 0)
    center_data = draw_center_data(jax.random.fold_in(streams_of[3], 71), 0)
    poly_coef = noise(streams_of[2], (COLS, 4), 0.5, 3.0, jnp.float32)
    return dict(fluid_data=fluid_data, center_data=center_data, poly_coef=poly_coef)


def kernel_block(center_pos, fluid_pos):
    dx = center_pos[0][:, None] - fluid_pos[0][None, :]
    dy = center_pos[1][:, None] - fluid_pos[1][None, :]
    dz = center_pos[2][:, None] - fluid_pos[2][None, :]
    sq = dx * dx + dy * dy + dz * dz
    phase = 2.0 * math.pi * WAVES * jnp.sqrt(sq)
    return jnp.sin(phase) / phase

def reference(fluid_data, center_data, poly_coef):
    total = center_data.shape[1]
    width = fluid_data.shape[1]
    block = math.gcd(total, 256)
    count = total // block
    fluid_pos = fluid_data[:3]
    forces = fluid_data[3:]
    pieces = center_data.reshape(center_data.shape[0], count, block).transpose(1, 0, 2)

    def step(motion, piece):
        tile = kernel_block(piece[:3], fluid_pos)
        motion = motion + jnp.dot(piece[3:], tile, precision=lax.Precision.HIGHEST, preferred_element_type=jnp.float32)
        back = lax.dot_general(forces, tile, (((1,), (1,)), ((), ())), precision=lax.Precision.HIGHEST, preferred_element_type=jnp.float32)
        return (motion, back)
    start = jnp.zeros((forces.shape[0], width), jnp.float32)
    motion, backs = lax.scan(step, start, pieces)
    loads = backs.transpose(1, 0, 2).reshape(forces.shape[0], total)
    affine = poly_coef[:, 0:1] + jnp.dot(poly_coef[:, 1:], fluid_pos, precision=lax.Precision.HIGHEST, preferred_element_type=jnp.float32)
    return (motion + affine, loads)
```

```python
import functools

import jax
import jax.numpy as jnp
from jax import lax
from jax.experimental import pallas as pl
from jax.experimental.pallas import tpu as pltpu
from jax.sharding import PartitionSpec as P

WAVES = 64
MESH = pl.DeviceIdType.MESH
TOP = 12.404427306735432
MID = 0.6418441597071612
LOW = 0.16126480593510223


def paired(me, m, n):
    if n & (n - 1) == 0:
        other, bit = 0, 1
        while bit < n:
            other = other + (((me // bit) % 2 + (m // bit) % 2) % 2) * bit
            bit *= 2
        return other, other
    return (me + m) % n, (me - m + n) % n


def dot(a, b, dims):
    return lax.dot_general(a, b, (dims, ((), ())), preferred_element_type=jnp.float32)


def split(x):
    high = x.astype(jnp.bfloat16)
    low = (x - high.astype(jnp.float32)).astype(jnp.bfloat16)
    return high, low


def body(rows, cols, side, fluid, center, poly, motion, loads, *scratch):
    fl, ce, cp, chl, fhl, kh, kl, mo_out, mo_in, ld_out, ld_in = scratch[:11]
    fs, fr, cs, cr, ms, mr, ls, lr = scratch[11:]
    S, T = cols // side, rows * side
    row, col = lax.axis_index("row"), lax.axis_index("col")
    my_s, my_t = col // side, (col % side) * rows + row
    nvals = poly.shape[0]
    wf, wc = fluid.shape[1], center.shape[1]
    lanes = 128 if wf % 128 == 0 else wf
    step_rows = 32 if wc % 32 == 0 else wc

    def along_s(m):
        to, src = paired(my_s, m, S)
        return tuple({"row": row, "col": i * side + col % side} for i in (to, src))

    def along_t(m):
        to, src = paired(my_t, m, T)
        return tuple({"row": i % rows, "col": (col // side) * side + i // rows} for i in (to, src))

    def copy(src, dst, send, recv, where):
        return pltpu.make_async_remote_copy(
            src_ref=src, dst_ref=dst, send_sem=send, recv_sem=recv, device_id=where, device_id_type=MESH
        )

    def send_fluid(m):
        return copy(fluid, fl.at[m], fs.at[m], fr.at[m], along_s(m)[0])

    def send_center(m):
        return copy(center, ce.at[m], cs.at[m], cr.at[m], along_t(m)[0])

    def send_motion(m):
        return copy(mo_out.at[m], mo_in.at[m], ms.at[m], mr.at[m], along_s(m)[1])

    def send_loads(m):
        return copy(ld_out.at[m], ld_in.at[m], ls.at[m], lr.at[m], along_t(m)[1])

    barrier = pltpu.get_barrier_semaphore()
    for m in range(1, max(S, T)):
        if m < T:
            pl.semaphore_signal(barrier, inc=1, device_id=along_t(m)[0], device_id_type=MESH)
        if m < S:
            pl.semaphore_signal(barrier, inc=1, device_id=along_s(m)[0], device_id_type=MESH)
    fl[0] = fluid[...]
    ce[0] = center[...]
    pl.semaphore_wait(barrier, S + T - 2)
    for m in range(1, max(S, T)):
        if m < T:
            send_center(m).start()
        if m < S:
            send_fluid(m).start()

    def ready_center(r):
        @pl.when(r > 0)
        def _():
            send_center(r).wait_recv()

        places = jnp.transpose(ce[r, 0:8, :] * float(WAVES))
        for a in range(3):
            cp[r, a] = jnp.broadcast_to(places[:, a : a + 1], (wc, lanes))
        high, low = split(ce[r, 3:, :] * TOP)
        chl[r, 0:nvals] = high
        chl[r, nvals:] = low
        ld_out[r] = jnp.zeros((nvals, wc), jnp.float32)

    def tile(m, r, slot):
        for h in range(wf // lanes):
            part = pl.ds(h * lanes, lanes)
            fx, fy, fz = (fl[m, a : a + 1, part] * float(WAVES) for a in range(3))
            for j in range(0, wc, step_rows):
                at = pl.ds(j, step_rows)
                dx, dy, dz = cp[r, 0, at, :] - fx, cp[r, 1, at, :] - fy, cp[r, 2, at, :] - fz
                sq = dx * dx + dy * dy + dz * dz
                inv = lax.rsqrt(sq)
                turns = sq * inv
                f = turns - jnp.round(turns)
                size = jnp.abs(f)
                rest = 0.5 - size
                q = size * rest
                value = (f * rest * inv) * ((q + MID) * q + LOW)
                high, low = split(value)
                kh[slot, at, part] = high
                kl[slot, at, part] = low
        k_high, k_low = kh[slot], kl[slot]
        across = ((1,), (0,))
        wide = dot(chl[r], k_high, across)
        mo_out[m] += wide[:nvals] + wide[nvals:] + dot(chl[r, 0:nvals], k_low, across)
        back = ((1,), (1,))
        wide = dot(fhl[...], k_high, back)
        ld_out[r] += wide[:nvals] + wide[nvals:] + dot(fhl[0:nvals], k_low, back)

    group = 2 if T % 2 == 0 else 1

    def step(s, _):
        m = (s + 1) % S
        last = s // (S - 1) if S > 1 else 1

        @pl.when(m > 0)
        def _():
            send_fluid(m).wait_recv()

        high, low = split(fl[m, 3:, :] * TOP)
        fhl[0:nvals] = high
        fhl[nvals:] = low
        mo_out[m] = jnp.zeros((nvals, wf), jnp.float32)

        def pair(k, _):
            which = [(k * group + e + last) % T for e in range(group)]

            @pl.when(s == 0)
            def _():
                for r in which:
                    ready_center(r)

            for e, r in enumerate(which):
                tile(m, r, e)

            @pl.when((s > 0) & (k == 0))
            def _():
                send_motion(s).start()

            for r in which:
                @pl.when((s == S - 1) & (r > 0))
                def _():
                    send_loads(r).start()

            return 0

        lax.fori_loop(0, T // group, pair, 0)
        return 0

    lax.fori_loop(0, S, step, 0)

    total = mo_out[0]
    for a in range(3):
        total = total + poly[:, a + 1 : a + 2] * fluid[a : a + 1, :]
    total = total + poly[:, 0:1]
    for m in range(1, S):
        send_motion(m).wait_recv()
        total = total + mo_in[m]
    motion[...] = total
    total = ld_out[0]
    for m in range(1, T):
        send_loads(m).wait_recv()
        total = total + ld_in[m]
    loads[...] = total
    for m in range(1, S):
        send_fluid(m).wait_send()
        send_motion(m).wait_send()
    for m in range(1, T):
        send_center(m).wait_send()
        send_loads(m).wait_send()


def per_device(rows, cols, side, fluid_data, center_data, poly_coef):
    f32, bf16 = jnp.float32, jnp.bfloat16
    S, T = cols // side, rows * side
    height, wf = fluid_data.shape
    wc = center_data.shape[1]
    n = height - 3
    lanes = 128 if wf % 128 == 0 else wf
    vmem = pl.BlockSpec(memory_space=pltpu.VMEM)
    sems = [pltpu.SemaphoreType.DMA((k,)) for k in (S, S, T, T, S, S, T, T)]
    return pl.pallas_call(
        functools.partial(body, rows, cols, side),
        out_shape=(jax.ShapeDtypeStruct((n, wf), f32), jax.ShapeDtypeStruct((n, wc), f32)),
        in_specs=[vmem] * 3,
        out_specs=(vmem, vmem),
        scratch_shapes=[
            pltpu.VMEM((S, height, wf), f32),
            pltpu.VMEM((T, height, wc), f32),
            pltpu.VMEM((T, 3, wc, lanes), f32),
            pltpu.VMEM((T, 2 * n, wc), bf16),
            pltpu.VMEM((2 * n, wf), bf16),
            pltpu.VMEM((2, wc, wf), bf16),
            pltpu.VMEM((2, wc, wf), bf16),
            pltpu.VMEM((S, n, wf), f32),
            pltpu.VMEM((S, n, wf), f32),
            pltpu.VMEM((T, n, wc), f32),
            pltpu.VMEM((T, n, wc), f32),
            *sems,
        ],
        compiler_params=pltpu.CompilerParams(
            collective_id=0, has_side_effects=True, vmem_limit_bytes=48 * 2**20
        ),
    )(fluid_data, center_data, poly_coef)


def solution(mesh):
    rows, cols = mesh.shape["row"], mesh.shape["col"]
    side = 2 if cols % 2 == 0 else 1
    placed = (P(None, ("row", "col")), P(None, ("col", "row")), P())
    return jax.shard_map(
        functools.partial(per_device, rows, cols, side),
        mesh=mesh,
        in_specs=placed,
        out_specs=(P(None, ("row", "col")), P(None, ("col", "row"))),
        check_vma=False,
    )
```

```python
import functools

import jax
import jax.numpy as jnp
from jax import lax
from jax.experimental import pallas as pl
from jax.experimental.pallas import tpu as pltpu
from jax.sharding import PartitionSpec as P

WAVES = 64
MESH = pl.DeviceIdType.MESH
TOP = 12.404427306735432
MID = 0.6418441597071612
LOW = 0.16126480593510223


def paired(me, m, n):
    other, bit = 0, 1
    while bit < n:
        other = other + (((me // bit) % 2 + (m // bit) % 2) % 2) * bit
        bit *= 2
    return other


def dot(a, b, dims):
    return lax.dot_general(a, b, (dims, ((), ())), preferred_element_type=jnp.float32)


def split(x):
    high = x.astype(jnp.bfloat16)
    low = (x - high.astype(jnp.float32)).astype(jnp.bfloat16)
    return high, low


def body(rows, cols, side, fluid, center, poly, motion, loads, *scratch):
    fl, ce, pv, cp, chl, fhl, kh, kl, mo_out, mo_in, ld_out, ld_in, pre = scratch[:13]
    own, fs, fr, cs, cr, ms, mr, ls, lr, ps, pr = scratch[13:]
    S, T = cols // side, rows * side
    half = T // 2
    row, col = lax.axis_index("row"), lax.axis_index("col")
    my_s, my_t = col // side, (row % 2) * half + (col % side) * (rows // 2) + row // 2
    nvals = pv.shape[1]
    wf, wc = fluid.shape[1], center.shape[1]
    lanes = 128 if wf % 128 == 0 else wf
    step_rows = 32 if wc % 32 == 0 else wc

    def along_s(m):
        return {"row": row, "col": paired(my_s, m, S) * side + col % side}

    def along_t(m):
        i = paired(my_t, m, T)
        return {
            "row": (i % (rows // 2)) * 2 + i // half,
            "col": (col // side) * side + (i % half) // (rows // 2),
        }

    def copy(src, dst, send, recv, where):
        return pltpu.make_async_remote_copy(
            src_ref=src, dst_ref=dst, send_sem=send, recv_sem=recv, device_id=where, device_id_type=MESH
        )

    def send_fluid(m):
        return copy(fl.at[0], fl.at[m], fs.at[m], fr.at[m], along_s(m))

    def send_center(p):
        return copy(ce.at[0], ce.at[p], cs.at[p], cr.at[p], along_t(half if p == 1 else p - 1))

    def hand_on(p):
        q = p + half - 1
        return copy(ce.at[p], ce.at[q], cs.at[q], cr.at[q], along_t(half))

    def send_motion(m):
        return copy(mo_out.at[m], mo_in.at[m], ms.at[m], mr.at[m], along_s(m))

    def send_pre(p):
        j = p - half
        return copy(ld_out.at[p], pre.at[j], ps.at[j], pr.at[j], along_t(half))

    def send_loads(j):
        return copy(ld_out.at[j + 1], ld_in.at[j], ls.at[j], lr.at[j], along_t(j))

    def send_other():
        return copy(ld_out.at[1], ld_in.at[0], ls.at[0], lr.at[0], along_t(half))

    local = [
        pltpu.make_async_copy(center, ce.at[0], own.at[0]),
        pltpu.make_async_copy(fluid, fl.at[0], own.at[1]),
        pltpu.make_async_copy(poly, pv, own.at[2]),
    ]
    for c in local:
        c.start()
    barrier = pltpu.get_barrier_semaphore()
    for p in range(1, half + 1):
        pl.semaphore_signal(barrier, inc=1, device_id=along_t(p), device_id_type=MESH)
    for m in range(1, S):
        pl.semaphore_signal(barrier, inc=1, device_id=along_s(m), device_id_type=MESH)
    for c in local:
        c.wait()
    order_s = [1] + list(range(S - 1, 1, -1))
    pl.semaphore_wait(barrier, S - 1 + half)
    for p in range(1, half + 1):
        send_center(p).start()
    for m in order_s:
        send_fluid(m).start()

    def ready_center(r):
        places = jnp.transpose(ce[r, 0:8, :] * float(WAVES))
        for a in range(3):
            cp[r, a] = jnp.broadcast_to(places[:, a : a + 1], (wc, lanes))
        high, low = split(ce[r, 3:, :] * TOP)
        chl[r, 0:nvals] = high
        chl[r, nvals:] = low
        ld_out[r] = jnp.zeros((nvals, wc), jnp.float32)

    def ready_fluid(m):
        high, low = split(fl[m, 3:, :] * TOP)
        fhl[m, 0:nvals] = high
        fhl[m, nvals:] = low
        mo_out[m] = jnp.zeros((nvals, wf), jnp.float32)

    def values(m, r, slot):
        for h in range(wf // lanes):
            part = pl.ds(h * lanes, lanes)
            fx, fy, fz = (fl[m, a : a + 1, part] * float(WAVES) for a in range(3))
            for j in range(0, wc, step_rows):
                at = pl.ds(j, step_rows)
                dx, dy, dz = cp[r, 0, at, :] - fx, cp[r, 1, at, :] - fy, cp[r, 2, at, :] - fz
                sq = dx * dx + dy * dy + dz * dz
                inv = lax.rsqrt(sq)
                turns = sq * inv
                f = turns - jnp.round(turns)
                size = jnp.abs(f)
                rest = 0.5 - size
                q = size * rest
                value = (f * rest * inv) * ((q + MID) * q + LOW)
                high, low = split(value)
                kh[slot, at, part] = high
                kl[slot, at, part] = low

    def sums(m, r, slot):
        k_high, k_low = kh[slot], kl[slot]
        across = ((1,), (0,))
        wide = dot(chl[r], k_high, across)
        mo_out[m] += wide[:nvals] + wide[nvals:] + dot(chl[r, 0:nvals], k_low, across)
        back = ((1,), (1,))
        wide = dot(fhl[m], k_high, back)
        ld_out[r] += wide[:nvals] + wide[nvals:] + dot(fhl[m, 0:nvals], k_low, back)

    def pair(before, one, two):
        sums(*before, 1)
        values(*one, 0)
        sums(*one, 0)
        values(*two, 1)
        return two

    kh[1] = jnp.zeros((wc, wf), jnp.bfloat16)
    kl[1] = jnp.zeros((wc, wf), jnp.bfloat16)
    ready_fluid(0)
    before = (0, 0)

    for k in range(half):
        for p in (2 * k, 2 * k + 1):
            if 2 <= p <= half:
                send_center(p).wait_recv()
                hand_on(p).start()
            elif p == 1:
                send_center(p).wait_recv()
            elif p > half:
                hand_on(p - half + 1).wait_recv()
            ready_center(p)
        if k == 0:
            send_fluid(order_s[0]).wait_recv()
            ready_fluid(order_s[0])
        m = order_s[0]
        before = pair(before, (m, 2 * k), (m, 2 * k + 1))

    def middle(s, _):
        m = S - s
        send_fluid(m).wait_recv()
        ready_fluid(m)
        last_m = (m + 1) % S + (m + 1) // S

        pair((last_m, T - 1), (m, 0), (m, 1))
        send_motion(last_m).start()

        def inner(k, _):
            pair((m, 2 * k - 1), (m, 2 * k), (m, 2 * k + 1))
            return 0

        lax.fori_loop(1, half, inner, 0)
        return 0

    lax.fori_loop(1, S - 2, middle, 0)

    far = order_s[-1]
    prior = order_s[-2]
    send_fluid(far).wait_recv()
    ready_fluid(far)
    pair((prior, T - 1), (far, T - 1), (0, T - 1))
    send_motion(prior).start()

    def mixed(k, _):
        r = T - 1 - k
        pair((0, r + 1), (far, r), (0, r))
        send_pre(r + 1).start()
        return 0

    lax.fori_loop(1, half, mixed, 0)

    def finish(j):
        send_pre(half + j).wait_recv()
        ld_out[j + 1] += pre[j]
        send_loads(j).start()

    pair((0, half), (far, half - 1), (far, half - 2))
    finish(half - 1)

    def far_rest(k, _):
        r = half - 1 - 2 * k
        pair((far, r + 1), (far, r), (far, r - 1))
        return 0

    lax.fori_loop(1, half // 2, far_rest, 0)
    pair((far, 0), (0, half - 1), (0, half - 2))
    send_motion(far).start()
    finish(half - 2)

    def own_rest(k, _):
        r = half - 1 - 2 * k
        pair((0, r + 1), (0, r), (0, r - 1))
        finish(r)

        @pl.when(r > 1)
        def _():
            finish(r - 1)

        return 0

    lax.fori_loop(1, half // 2, own_rest, 0)
    send_other().start()
    sums(0, 0, 1)

    total = mo_out[0]
    affine = jnp.transpose(pv[...])
    for a in range(3):
        total = total + affine[:, a + 1 : a + 2] * fl[0, a : a + 1, :]
    total = total + affine[:, 0:1]
    for m in order_s:
        send_motion(m).wait_recv()
        total = total + mo_in[m]
    motion[...] = total
    total = ld_out[0]
    for j in range(half - 1, 0, -1):
        send_loads(j).wait_recv()
        total = total + ld_in[j]
    send_other().wait_recv()
    loads[...] = total + ld_in[0]
    for m in order_s:
        send_fluid(m).wait_send()
        send_motion(m).wait_send()
    for p in range(1, half + 1):
        send_center(p).wait_send()
    for p in range(2, half + 1):
        hand_on(p).wait_send()
        send_pre(p + half - 1).wait_send()
        send_loads(p - 1).wait_send()
    send_other().wait_send()


def per_device(rows, cols, side, fluid_data, center_data, poly_coef):
    f32, bf16 = jnp.float32, jnp.bfloat16
    S, T = cols // side, rows * side
    height, wf = fluid_data.shape
    wc = center_data.shape[1]
    n = height - 3
    lanes = 128 if wf % 128 == 0 else wf
    vmem = pl.BlockSpec(memory_space=pltpu.VMEM)
    hbm = pl.BlockSpec(memory_space=pltpu.HBM)
    sems = [pltpu.SemaphoreType.DMA((k,)) for k in (3, S, S, T, T, S, S, T // 2, T // 2, T // 2, T // 2)]
    return pl.pallas_call(
        functools.partial(body, rows, cols, side),
        out_shape=(jax.ShapeDtypeStruct((n, wf), f32), jax.ShapeDtypeStruct((n, wc), f32)),
        in_specs=[hbm] * 3,
        out_specs=(vmem, vmem),
        scratch_shapes=[
            pltpu.VMEM((S, height, wf), f32),
            pltpu.VMEM((T, height, wc), f32),
            pltpu.VMEM((4, n), f32),
            pltpu.VMEM((T, 3, wc, lanes), f32),
            pltpu.VMEM((T, 2 * n, wc), bf16),
            pltpu.VMEM((S, 2 * n, wf), bf16),
            pltpu.VMEM((2, wc, wf), bf16),
            pltpu.VMEM((2, wc, wf), bf16),
            pltpu.VMEM((S, n, wf), f32),
            pltpu.VMEM((S, n, wf), f32),
            pltpu.VMEM((T, n, wc), f32),
            pltpu.VMEM((T // 2, n, wc), f32),
            pltpu.VMEM((T // 2, n, wc), f32),
            *sems,
        ],
        compiler_params=pltpu.CompilerParams(
            collective_id=0, has_side_effects=True, vmem_limit_bytes=48 * 2**20
        ),
    )(fluid_data, center_data, poly_coef.T)


def solution(mesh):
    rows, cols = mesh.shape["row"], mesh.shape["col"]
    side = 2 if cols % 2 == 0 else 1
    placed = (P(None, ("row", "col")), P(None, ("col", "row")), P())
    return jax.shard_map(
        functools.partial(per_device, rows, cols, side),
        mesh=mesh,
        in_specs=placed,
        out_specs=(P(None, ("row", "col")), P(None, ("col", "row"))),
        check_vma=False,
    )
```
